32 devices in a mesh: group: 1, stream: 16 (over z, y, x), expert: 2 (over core).
Axes of the slice: x: 2, y: 2, z: 4, core: 2. Of those that a mesh axis runs over, the one named last changes fastest.
Arguments:
- hidden_in: bfloat16 [512, 4096], P(('group', 'stream', 'expert')), may hold values from -6 to 6
- routes: int32 [512, 2], P(('group', 'stream', 'expert')), may hold values from 0 to 3, all different within a row; in each aligned block of 512 rows (0 to 511, 512 to 1023, ...) at most 384 rows name the same one
- norm_gain: float32 [4096], replicated, may hold values from 0.25 to 1.75
- router: bfloat16 [4096, 4], replicated, may hold values from -0.1875 to 0.1875
- w_gate: bfloat16 [4, 4096, 7168], P('expert', None, 'stream'), may hold values from -0.09375 to 0.09375
- w_up: bfloat16 [4, 4096, 7168], P('expert', None, 'stream'), may hold values from -0.09375 to 0.09375
- w_down: bfloat16 [4, 7168, 4096], P('expert', 'stream'), may hold values from -0.0625 to 0.0625
Outputs:
- hidden_out: bfloat16 [512, 4096], P(('group', 'stream', 'expert'))
The draws below stay inside these ranges and needn't reach their ends.
Inputs may be any that keep to these rules, and one draw needn't show every extreme that they name: `routes`: each token names two different experts; no expert is named by more than 384 tokens of a replica, a bound that some block reaches.
All inputs are finite; a program needn't handle non-finite values.
Results may differ from the reference program's by a relative error of at most 0.006.
Values may be sent and summed in bfloat16 or wider, within the bound.
No kernel may reach another device: no remote copies, remote signals or barrier semaphores. Data moves between devices by JAX's collectives and lax.ppermute only.
A program may use at most 192 MiB of HBM per device.

```python
import math
import jax
import jax.numpy as jnp
import numpy as np
from jax import lax

D = 4096
FF = 7168
EXPERTS = 4
TOKENS = 512
CAP = 384


def shard_levels(stream_key, shape, shards, smallest, top_value):
    loudness = 1.0
    for dim, shards_of in shards:
        steps = jax.random.uniform(jax.random.fold_in(jax.random.fold_in(stream_key, 6), dim), (shards_of,), jnp.float32, smallest / len(shards), top_value / len(shards))
        loudness = loudness * jnp.repeat(jnp.exp(steps), shape[dim] // shards_of).reshape((-1,) + (1,) * (len(shape) - 1 - dim))
    return loudness


def assign_block(stream_key, own, number, rows, number_of, top, bound, skew):
    ranking = jax.random.permutation(stream_key, number_of)
    crowded, ordinary = shares(number_of, rows * top, bound, skew, True), shares(number_of, rows * top, bound, skew, False)
    places = jnp.arange(number_of)

    def named(tallies, rotation):
        used = int((tallies > 0).sum())
        fixed = max(1, used // 4)
        passed = fixed + (places - fixed + rotation * (used - fixed)) % max(1, number_of - fixed)
        return jnp.zeros((number_of,), jnp.int32).at[ranking[jnp.where(places < fixed, places, passed)]].set(jnp.asarray(tallies, jnp.int32))

    tallies = jnp.where(number % 4 == 0, named(crowded, number // 4), named(ordinary, number - number // 4 - 1))
    mixed = jax.random.permutation(jax.random.fold_in(own, 3), number_of)
    source_of, receiver = mixed[0:number_of // 2 * 2:2], mixed[1:number_of // 2 * 2:2]
    slack = jnp.minimum(tallies[source_of] - 1, bound - tallies[receiver]) // 2
    slack = jnp.where((source_of == ranking[0]) | (receiver == ranking[0]) | (tallies[receiver] == 0), 0, jnp.maximum(slack, 0))
    passed = jax.random.randint(jax.random.fold_in(own, 4), (number_of // 2,), 0, 1 << 20) % (slack + 1)
    tallies = tallies.at[source_of].add(-passed).at[receiver].add(passed)
    items = jnp.searchsorted(jnp.cumsum(tallies), jnp.arange(rows * top), side="right").astype(jnp.int32)
    listing = items.reshape(top, rows).T
    listing = listing[jax.random.permutation(jax.random.fold_in(own, 1), rows)]
    rotation = jax.random.randint(jax.random.fold_in(own, 2), (rows, 1), 0, top)
    return jnp.take_along_axis(listing, (jnp.arange(top)[None, :] + rotation) % top, axis=1)


def shares(count, total, bound, slope, full):
    weights = [(1 << 20) // math.isqrt(standing ** slope) + 1 for standing in range(1, count + 1)]
    largest = bound if full else min(bound, max(-(-total // count), total * weights[0] // sum(weights)))
    least = 1 if total - largest >= count - 1 else 0
    given, surplus = [largest] + [least] * (count - 1), total - largest - least * (count - 1)
    while surplus > 0:
        free = [i for i in range(1, count) if given[i] < largest] or [i for i in range(1, count) if given[i] < bound]
        whole, budget = sum([weights[i] for i in free]), surplus
        for i in free:
            addition = min(bound - given[i], max(1, budget * weights[i] // whole), surplus)
            given[i] = given[i] + addition
            surplus = surplus - addition
    return np.array(given)


def bell_draw(key, shape, scale, bound, pieces=(), kind=jnp.bfloat16):
    array = jax.random.normal(key, shape, jnp.float32) * scale
    if len(pieces) > 0:
        array = shard_levels(key, shape, pieces, -0.22, 0.18) * array
    return jnp.clip(array, min=-bound, max=bound).astype(kind)


def setup_inputs(seed: int = 0, part: int = 0) -> dict:
    streams_of = jax.random.split(jax.random.key(seed), 8)
    own_keys = jax.random.split(jax.random.fold_in(streams_of[7], part), 8)
    hidden_in = bell_draw(own_keys[0], (TOKENS, D), 1.0, 6.0, ((0, 32),))
    routes_keys = jax.random.split(jax.random.fold_in(own_keys[1], 1), TOKENS // TOKENS)
    routes_turns = jax.random.permutation(jax.random.fold_in(own_keys[1], 3), TOKENS // TOKENS)
    routes = jax.vmap(lambda own, number: assign_block(jax.random.fold_in(own_keys[1], 2), own, number, TOKENS, EXPERTS, 2, CAP, 1))(routes_keys, routes_turns).reshape((TOKENS, 2))
    norm_gain = jnp.clip(1.0 + 0.15 * jax.random.normal(streams_of[2], (D,), jnp.float32), 0.25, 1.75)
    router = bell_draw(streams_of[3], (D, EXPERTS), (D // 4) ** -0.5, 0.1875)
    w_gate = bell_draw(streams_of[4], (EXPERTS, D, FF), D ** -0.5, 0.09375, ((0, 2), (2, 16)))
    w_up = bell_draw(streams_of[5], (EXPERTS, D, FF), D ** -0.5, 0.09375, ((0, 2), (2, 16)))
    w_down = bell_draw(streams_of[6], (EXPERTS, FF, D), FF ** -0.5, 0.0625, ((0, 2), (1, 16)))
    return {"hidden_in": hidden_in, "routes": routes, "norm_gain": norm_gain, "router": router, "w_gate": w_gate, "w_up": w_up, "w_down": w_down}


EPS = 1e-05

def route_table(normed, routes, router):
    logits = jnp.dot(normed, router, preferred_element_type=jnp.float32)
    picked = jnp.take_along_axis(logits, routes, axis=1)
    first_weight = 1.0 / (1.0 + jnp.exp(picked[:, 1] - picked[:, 0]))
    second_weight = 1.0 - first_weight
    experts = jnp.arange(router.shape[1], dtype=jnp.int32)
    table = jnp.where(routes[:, 0:1] == experts, first_weight[:, None], jnp.zeros((), jnp.float32))
    table = table + jnp.where(routes[:, 1:2] == experts, second_weight[:, None], jnp.zeros((), jnp.float32))
    return table.astype(jnp.bfloat16)

def reference(hidden_in, routes, norm_gain, router, w_gate, w_up, w_down):
    own_rows = hidden_in.astype(jnp.float32)
    mean_sq = lax.optimization_barrier(jnp.mean(own_rows * own_rows, axis=1, keepdims=True))
    normed = (own_rows * lax.rsqrt(mean_sq + EPS) * norm_gain).astype(jnp.bfloat16)
    route_weights = route_table(normed, routes, router)
    row_total = normed.shape[0]
    position = jnp.arange(row_total, dtype=jnp.int32)
    mixture = jnp.zeros(own_rows.shape, jnp.float32)
    for expert_slot in range(EXPERTS):
        weight = route_weights[:, expert_slot].astype(jnp.float32)
        sort_keys = jnp.where(weight > 0, position, position + row_total)
        chosen = jnp.argsort(sort_keys)[:CAP]
        rows = normed[chosen]
        gate_proj = jnp.dot(rows, w_gate[expert_slot], preferred_element_type=jnp.float32)
        up_proj = jnp.dot(rows, w_up[expert_slot], preferred_element_type=jnp.float32)
        activated = (jax.nn.silu(gate_proj) * up_proj).astype(jnp.bfloat16)
        expert_out = jnp.dot(activated, w_down[expert_slot], preferred_element_type=jnp.float32)
        mixture = mixture.at[chosen].add(expert_out * weight[chosen][:, None])
    return (own_rows + mixture).astype(jnp.bfloat16)
```

```python
import functools

import jax
import jax.numpy as jnp
from jax import lax
from jax.experimental import pallas as pl
from jax.experimental.pallas import tpu as pltpu
from jax.sharding import PartitionSpec as P

EPS = 1e-05
LANES = 128
NT = (((1,), (1,)), ((), ()))


def prologue_kernel(widths, hidden_hbm, routes_hbm, gain_hbm, router_hbm, *refs):
    outs, (hidden_ref, routes_ref, gain_ref, router_ref, sems) = refs[:-5], refs[-5:]
    copies = [
        pltpu.make_async_copy(src, dst, sems.at[i])
        for i, (src, dst) in enumerate(
            (
                (hidden_hbm, hidden_ref),
                (gain_hbm, gain_ref),
                (router_hbm, router_ref),
                (routes_hbm, routes_ref),
            )
        )
    ]
    for copy in copies:
        copy.start()
    copies[0].wait()
    copies[1].wait()
    rows = hidden_ref[...].astype(jnp.float32)
    mean_sq = jnp.mean(rows * rows, axis=1, keepdims=True)
    normed = (rows * lax.rsqrt(mean_sq + EPS) * gain_ref[...]).astype(jnp.bfloat16)
    start = 0
    for out, width in zip(outs, widths):
        out[:, :width] = normed[:, start : start + width]
        start += width
    copies[2].wait()
    copies[3].wait()
    logits = lax.dot_general(normed, router_ref[...], NT, preferred_element_type=jnp.float32)
    count = rows.shape[0]
    eye = (
        lax.broadcasted_iota(jnp.int32, (count, count), 0)
        == lax.broadcasted_iota(jnp.int32, (count, count), 1)
    ).astype(jnp.float32)
    picks = lax.dot_general(
        eye, routes_ref[...].astype(jnp.float32), NT, preferred_element_type=jnp.float32
    )
    experts = lax.broadcasted_iota(jnp.int32, logits.shape, 1).astype(jnp.float32)
    first = jnp.abs(picks[:, 0:1] - experts) < 0.5
    second = jnp.abs(picks[:, 1:2] - experts) < 0.5
    a = jnp.sum(jnp.where(first, logits, 0.0), axis=1, keepdims=True)
    b = jnp.sum(jnp.where(second, logits, 0.0), axis=1, keepdims=True)
    first_weight = 1.0 / (1.0 + jnp.exp(b - a))
    table = jnp.where(first, first_weight, 0.0) + jnp.where(second, 1.0 - first_weight, 0.0)
    last = outs[-1]
    last[:, widths[-1] :] = jnp.zeros((count, LANES), last.dtype)
    last[:, widths[-1] : widths[-1] + table.shape[1]] = table.astype(last.dtype)


def prologue(hidden_in, routes, norm_gain, router, widths):
    rows, features = hidden_in.shape
    full = list(widths)
    full[-1] += LANES
    gain = norm_gain.reshape(1, features)
    operands = (hidden_in, routes.T, gain, router.T)
    return pl.pallas_call(
        functools.partial(prologue_kernel, widths),
        in_specs=[pl.BlockSpec(memory_space=pltpu.HBM)] * 4,
        out_shape=[jax.ShapeDtypeStruct((rows, w), jnp.bfloat16) for w in full],
        scratch_shapes=[
            pltpu.VMEM(hidden_in.shape, hidden_in.dtype),
            pltpu.VMEM(operands[1].shape, routes.dtype),
            pltpu.VMEM(gain.shape, gain.dtype),
            pltpu.VMEM(operands[3].shape, router.dtype),
            pltpu.SemaphoreType.DMA((4,)),
        ],
        compiler_params=pltpu.CompilerParams(vmem_limit_bytes=8 * 2**20),
        name="prologue",
    )(*operands)


def stack_kernel(widths, *refs):
    pieces, outs = refs[: -len(widths)], refs[-len(widths) :]
    row = 0
    for piece in pieces:
        start = 0
        for out, width in zip(outs, widths):
            out[row : row + piece.shape[0], :] = piece[:, start : start + width]
            start += width
        row += piece.shape[0]


def stack(pieces, widths):
    rows = sum(p.shape[0] for p in pieces)
    return pl.pallas_call(
        functools.partial(stack_kernel, widths),
        out_shape=[jax.ShapeDtypeStruct((rows, w), pieces[0].dtype) for w in widths],
        compiler_params=pltpu.CompilerParams(vmem_limit_bytes=8 * 2**20),
        name="stack",
    )(*pieces)


def gate_up_kernel(layout, rows, core_ref, *refs):
    pieces, refs = refs[: len(layout)], refs[len(layout) :]
    gate_ref, up_ref, h_ref, x_ref, table_ref = refs
    local = gate_ref.shape[0]
    features = gate_ref.shape[2]
    for piece, (group, stride, column, width) in zip(pieces, layout):
        for i in range(piece.shape[0] // rows):
            at = (group + i * stride) * rows
            block = slice(i * rows, (i + 1) * rows)
            x_ref[at : at + rows, column : column + width] = piece[block, :width]
            if column + width == features:
                table_ref[at : at + rows, :] = piece[block, width:].astype(jnp.float32)
    lane0 = core_ref[0] * local
    tile = 256

    @pl.loop(0, x_ref.shape[0] // tile)
    def _(m):
        block = pl.ds(pl.multiple_of(m * tile, tile), tile)
        x = x_ref[block, :]
        table = table_ref[block, :]
        lanes = lax.broadcasted_iota(jnp.int32, table.shape, 1)
        for e in range(local):
            weight = jnp.sum(jnp.where(lanes == lane0 + e, table, 0.0), axis=1, keepdims=True)
            gate = lax.dot_general(x, gate_ref[e], NT, preferred_element_type=jnp.float32)
            up = lax.dot_general(x, up_ref[e], NT, preferred_element_type=jnp.float32)
            value = gate / (1.0 + jnp.exp(-gate)) * up * weight
            h_ref[e, block, :] = value.astype(h_ref.dtype)


def gate_up(core, pieces, layout, rows, tokens, w_gate, w_up):
    local, hidden, features = w_gate.shape
    return pl.pallas_call(
        functools.partial(gate_up_kernel, layout, rows),
        in_specs=[pl.BlockSpec(memory_space=pltpu.SMEM)]
        + [pl.BlockSpec(memory_space=pltpu.VMEM)] * (len(pieces) + 2),
        out_shape=jax.ShapeDtypeStruct((local, tokens, hidden), jnp.bfloat16),
        scratch_shapes=[
            pltpu.VMEM((tokens, features), jnp.bfloat16),
            pltpu.VMEM((tokens, LANES), jnp.float32),
        ],
        compiler_params=pltpu.CompilerParams(vmem_limit_bytes=16 * 2**20),
        cost_estimate=pl.CostEstimate(
            flops=4 * tokens * features * local * hidden,
            bytes_accessed=4 * local * hidden * features,
            transcendentals=0,
        ),
        name="gate_up",
    )(core, *pieces, w_gate, w_up)


def down_kernel(start, order, rows, h_ref, w_ref, own_ref, other_ref):
    tile = 512
    own = own_ref.shape[0]
    for column in range(0, own_ref.shape[1], tile):
        cut = slice(start + column, start + column + tile)
        total = jnp.dot(h_ref[0], w_ref[0, :, cut], preferred_element_type=jnp.float32)
        for e in range(1, h_ref.shape[0]):
            total += jnp.dot(h_ref[e], w_ref[e, :, cut], preferred_element_type=jnp.float32)
        here = slice(column, column + tile)
        for at, source in enumerate(order):
            block = slice(at * rows, (at + 1) * rows)
            own_ref[block, here] = total[source * rows : (source + 1) * rows]
            other_ref[block, here] = total[own + source * rows : own + (source + 1) * rows].astype(
                other_ref.dtype
            )


def down(h, w_down, start, width, order, rows):
    local, tokens, hidden = h.shape
    own = tokens // 2
    return pl.pallas_call(
        functools.partial(down_kernel, start, order, rows),
        in_specs=[pl.BlockSpec(memory_space=pltpu.VMEM)] * 2,
        out_shape=[
            jax.ShapeDtypeStruct((own, width), jnp.float32),
            jax.ShapeDtypeStruct((own, width), jnp.bfloat16),
        ],
        compiler_params=pltpu.CompilerParams(vmem_limit_bytes=16 * 2**20),
        cost_estimate=pl.CostEstimate(
            flops=2 * tokens * width * local * hidden,
            bytes_accessed=2 * local * hidden * width,
            transcendentals=0,
        ),
        name="down",
    )(h, w_down)


def body(stream_count, core_count, hidden_in, routes, norm_gain, router, w_gate, w_up, w_down):
    rows, features = hidden_in.shape
    z_count = stream_count // 4

    def swap_stream(x, mask):
        return lax.ppermute(x, "stream", [(i, i ^ mask) for i in range(stream_count)])

    def swap_core(x):
        return lax.ppermute(x, "expert", [(i, i ^ 1) for i in range(core_count)])

    swap_x = lambda v: swap_stream(v, 1)
    swap_y = lambda v: swap_stream(v, 2)
    swaps_z = lambda v: [swap_stream(v, 4 * k) for k in range(1, z_count)]
    tail = features // 4
    part = (features - tail) // 2
    core = lax.axis_index("expert").astype(jnp.int32).reshape(1)
    plane = z_count * rows
    own_rows = stream_count * rows
    bf16 = lambda v: v.astype(jnp.bfloat16)
    f32 = lambda v: v.astype(jnp.float32)

    main, rest = prologue(hidden_in, routes, norm_gain, router, (2 * part, tail))
    from_z = swaps_z(main)
    rest_x, rest_y = swap_x(rest), swap_y(rest)
    rest_corner = swap_x(rest_y)
    (rest_plane,) = stack([rest, rest_x, rest_y, rest_corner], (tail + LANES,))
    first, second = stack([main] + from_z, (part, part))
    first_y, second_x = swap_y(first), swap_x(second)
    first_x, second_y = swap_x(first), swap_y(second)
    first_corner, second_corner = swap_x(first_y), swap_y(second_x)
    rest_z = [rest_plane] + swaps_z(rest_plane)
    pieces, layout = [], []
    for column, blocks in (
        (0, (first, first_x, first_y, first_corner)),
        (part, (second, second_x, second_y, second_corner)),
    ):
        for place, block in enumerate(blocks):
            for side, piece in enumerate((block, swap_core(block))):
                pieces.append(piece)
                layout.append((side * stream_count + place * z_count, 1, column, part))
    for z, block in enumerate(rest_z):
        for side, piece in enumerate((block, swap_core(block))):
            pieces.append(piece)
            layout.append((side * stream_count + z, z_count, 2 * part, tail))

    h = gate_up(
        core,
        pieces,
        tuple(layout),
        rows,
        core_count * own_rows,
        w_gate.transpose(0, 2, 1),
        w_up.transpose(0, 2, 1),
    )

    straight = tuple(range(stream_count))
    by_z = tuple(place * z_count + z for z in range(z_count) for place in range(4))

    def summed(start, width, order):
        mine, theirs = down(h, w_down, start, width, order, rows)
        return mine, swap_core(theirs)

    def cut(pair, i, size):
        return pair[0][i * size : (i + 1) * size] + f32(pair[1][i * size : (i + 1) * size])

    one, two = summed(0, part, straight), summed(part, part, straight)
    last = summed(2 * part, tail, by_z)
    one_corner = swap_x(bf16(cut(one, 3, plane)))
    two_corner = swap_y(bf16(cut(two, 3, plane)))
    one_x, two_y = swap_x(bf16(cut(one, 1, plane))), swap_y(bf16(cut(two, 2, plane)))
    one_y = swap_y(bf16(cut(one, 2, plane) + f32(one_corner)))
    two_x = swap_x(bf16(cut(two, 1, plane) + f32(two_corner)))
    one_sum = cut(one, 0, plane) + f32(one_x) + f32(one_y)
    two_sum = cut(two, 0, plane) + f32(two_x) + f32(two_y)
    both = jnp.concatenate([one_sum, two_sum], axis=1)
    mixture = both[:rows]
    for k in range(1, z_count):
        mixture = mixture + f32(swap_stream(bf16(both[k * rows : (k + 1) * rows]), 4 * k))

    last_plane = cut(last, 0, 4 * rows)
    for k in range(1, z_count):
        last_plane = last_plane + f32(swap_stream(bf16(cut(last, k, 4 * rows)), 4 * k))
    last_corner = swap_x(bf16(last_plane[3 * rows :]))
    last_x = swap_x(bf16(last_plane[rows : 2 * rows]))
    last_y = swap_y(bf16(last_plane[2 * rows : 3 * rows] + f32(last_corner)))
    last_mixture = last_plane[:rows] + f32(last_x) + f32(last_y)
    mixture = jnp.concatenate([mixture, last_mixture], axis=1)
    return bf16(f32(hidden_in) + mixture)


def solution(mesh):
    return jax.shard_map(
        functools.partial(body, mesh.shape["stream"], mesh.shape["expert"]),
        mesh=mesh,
        in_specs=(
            P(("group", "stream", "expert"), None),
            P(("group", "stream", "expert"), None),
            P(),
            P(),
            P("expert", None, "stream"),
            P("expert", None, "stream"),
            P("expert", "stream", None),
        ),
        out_specs=P(("group", "stream", "expert"), None),
        check_vma=False,
    )
```
